32 devices in a mesh: dp: 8 (over z, y), tp: 4 (over x, core).
Axes of the slice: x: 2, y: 2, z: 4, core: 2. Of those that a mesh axis runs over, the one named last changes fastest.
Arguments:
- q_latent: bfloat16 [1024, 4, 1536], P('dp'), may hold values from -6 to 6
- new_latent: bfloat16 [1024, 4, 512], P('dp'), may hold values from -6 to 6
- new_rope: bfloat16 [1024, 4, 64], P('dp'), may hold values from -6 to 6
- cache_latent: bfloat16 [1024, 256, 512], P('dp'), may hold values from -6 to 6
- cache_rope: bfloat16 [1024, 64, 256], P('dp'), may hold values from -1200 to 1200
- lengths: int32 [1024], P('dp'), may hold values from 1 to 256
- assignment: int32 [8, 128], P('dp'), may hold values from 0 to 127, each once within a row
- w_uq: float32 [1536, 12288], P(('dp', 'tp')), may hold values from -0.15625 to 0.15625
- w_uk: float32 [512, 8192], P(('dp', 'tp')), may hold values from -0.75 to 0.75
- w_uv: float32 [512, 8192], P(('dp', 'tp')), may hold values from -0.25 to 0.25
- w_o: float32 [8192, 7168], P(None, ('dp', 'tp')), may hold values from -0.0625 to 0.0625
Outputs:
- attention_out: bfloat16 [1024, 4, 7168], P('dp', None, 'tp')
- weight_norm: float32 [1], replicated
The draws below stay inside these ranges and needn't reach their ends.
Inputs may be any that keep to these rules, and one draw needn't show every extreme that they name: Each row of assignment is a permutation of 0 to 127.
All inputs are finite; a program needn't handle non-finite values.
Results may differ from the reference program's by a relative error of at most 0.006.
The reference program's roundings to bfloat16 on the way count: a program that leaves them out, or rounds other values in their place, can miss the bound.
Values may be sent and summed in bfloat16 or wider, within the bound.
A program may use at most 256 MiB of HBM per device.

```python
import jax
import jax.numpy as jnp
from jax import lax

D = 7168
QRANK = 1536
KVRANK = 512
NOPE = 128
ROPE = 64
VDIM = 128
HEADS = 64
NEWTOK = 4
SEQ_REP = 128
CACHE = 256
REPLICAS = 8
SEQS = 1024


def draw_cache_rope(key, part):
    values = jnp.clip(jax.random.normal(key, (SEQS, ROPE, CACHE), jnp.float32), -4.0, 4.0)
    return values.astype(jnp.bfloat16)


def place_ends(entries, stream_key, least, top_value):
    spot = [jax.random.randint(jax.random.fold_in(stream_key, axis), (), 0, length) for axis, length in enumerate(entries.shape)]
    longest = entries.shape.index(max(entries.shape))
    next_to = spot[:longest] + [(spot[longest] + 1) % entries.shape[longest]] + spot[longest + 1:]
    return entries.at[tuple(spot)].set(least).at[tuple(next_to)].set(top_value)


def strengthened(entries, rng, source, target, shards_of, factor):
    owner, partner = [(jnp.arange(entries.shape[position]) // (entries.shape[position] // shards_of)).reshape([-1 if axis == position else 1 for axis in range(entries.ndim)]) for position in (source, target)]
    chosen = jax.random.permutation(rng, shards_of)[partner]
    strong = (owner == chosen) | (owner == (partner + shards_of // 2) % shards_of)
    return jnp.where(strong, factor * entries, entries)


def level_of(rng, dims, cuts, smallest, top_value):
    gain, own = 1.0, jax.random.fold_in(rng, 6)
    for axis_at, shards_of in cuts:
        heights = jnp.exp(jax.random.uniform(jax.random.fold_in(own, axis_at), (shards_of,), jnp.float32, smallest / len(cuts), top_value / len(cuts)))
        gain = gain * jnp.repeat(heights, dims[axis_at] // shards_of).reshape([-1 if axis == axis_at else 1 for axis in range(len(dims))])
    return gain


def noise(stream_key, extent, width, reach, pieces=(), held_as=jnp.bfloat16):
    entries = jax.random.normal(stream_key, extent, jnp.float32) * width
    if len(pieces) > 0:
        entries = level_of(stream_key, extent, pieces, -0.22, 0.18) * entries
    return jnp.clip(entries, min=-reach, max=reach).astype(held_as)


def heavy_noise(own_key, shape, deviation, bound, split, heavy, held_as=jnp.bfloat16):
    entries = deviation * jax.random.normal(own_key, shape, jnp.float32)
    if split:
        entries = entries * level_of(own_key, shape, split, -0.22, 0.18)
    return jnp.clip(strengthened(entries, jax.random.fold_in(own_key, 3), *heavy), -bound, bound).astype(held_as)


def setup_inputs(seed: int = 0) -> dict:
    arg_keys = jax.random.split(jax.random.key(seed), 12)
    return {
        "q_latent": noise(arg_keys[0], (SEQS, NEWTOK, QRANK), 1.0, 6.0, ((0, 8),)),
        "new_latent": noise(arg_keys[1], (SEQS, NEWTOK, KVRANK), 1.0, 6.0, ((0, 8),)),
        "new_rope": noise(arg_keys[2], (SEQS, NEWTOK, ROPE), 1.0, 6.0, ((0, 8),)),
        "cache_latent": noise(arg_keys[3], (SEQS, CACHE, KVRANK), 1.0, 6.0, ((0, 8),)),
        "cache_rope": draw_cache_rope(jax.random.fold_in(arg_keys[11], 71), 0),
        "lengths": place_ends(jax.random.randint(arg_keys[5], (SEQS,), 1, CACHE + 1), jax.random.fold_in(arg_keys[5], 1), 1, CACHE).astype(jnp.int32),
        "assignment": jax.vmap(lambda own: jax.random.permutation(own, SEQ_REP))(jax.random.split(arg_keys[6], REPLICAS)).reshape((REPLICAS, SEQ_REP)).astype(jnp.int32),
        "w_uq": noise(arg_keys[7], (QRANK, HEADS * (NOPE + ROPE)), QRANK ** -0.5, 0.15625, ((0, 32),), jnp.float32),
        "w_uk": heavy_noise(arg_keys[8], (KVRANK, HEADS * NOPE), 0.125, 0.75, ((0, 32),), (0, 1, 32, 2.75), jnp.float32),
        "w_uv": noise(arg_keys[9], (KVRANK, HEADS * VDIM), KVRANK ** -0.5, 0.25, ((0, 32),), jnp.float32),
        "w_o": noise(arg_keys[10], (HEADS * VDIM, D), (HEADS * VDIM) ** -0.5, 0.0625, ((1, 32),), jnp.float32),
    }


def widen(values):
    return lax.optimization_barrier(values).astype(jnp.float32)

def rotate_half(values, positions):
    half_width = values.shape[-1] // 2
    frequency = 10000.0 ** (-jnp.arange(half_width, dtype=jnp.float32) / half_width)
    angles = positions.astype(jnp.float32)[:, :, None, None] * frequency
    cosine = jnp.cos(angles)
    sine_part = jnp.sin(angles)
    lower_half = values[..., :half_width]
    upper_half = values[..., half_width:]
    return jnp.concatenate([lower_half * cosine - upper_half * sine_part, upper_half * cosine + lower_half * sine_part], axis=-1)

def reference(q_latent, new_latent, new_rope, cache_latent, cache_rope, lengths, assignment, w_uq, w_uk, w_uv, w_o):
    high = lax.Precision.HIGHEST
    squares_total = jnp.sum(w_uq * w_uq) + jnp.sum(w_uk * w_uk) + jnp.sum(w_uv * w_uv) + jnp.sum(w_o * w_o)
    weight_norm = jnp.sqrt(squares_total / (HEADS * (NOPE + ROPE) + 2 * HEADS * NOPE + D)).reshape(1)
    query_up = w_uq.astype(jnp.bfloat16)
    key_up = widen(w_uk.astype(jnp.bfloat16)).reshape(KVRANK, HEADS, NOPE)
    value_up = widen(w_uv.astype(jnp.bfloat16)).reshape(KVRANK, HEADS, VDIM)
    out_proj = w_o.astype(jnp.bfloat16)
    scale = (NOPE + ROPE) ** (-0.5)

    def replica(inputs):
        queries, latents, ropes, cache_lat, cache_rot, lens, order = inputs
        slot_lat = widen(cache_lat[order])
        slot_rot = widen(cache_rot[order])
        slot_len = lens[order]
        projected = jnp.dot(queries.reshape(SEQ_REP * NEWTOK, QRANK), query_up, preferred_element_type=jnp.float32)
        projected = projected.astype(jnp.bfloat16).reshape(SEQ_REP, NEWTOK, HEADS, NOPE + ROPE)
        query_nope = widen(projected[..., :NOPE])
        positions = slot_len[:, None] + jnp.arange(NEWTOK, dtype=jnp.int32)[None, :]
        query_rot = widen(rotate_half(widen(projected[..., NOPE:]), positions).astype(jnp.bfloat16))
        absorbed = jnp.einsum('sqhn,chn->sqhc', query_nope, key_up, precision=high).astype(jnp.bfloat16)
        absorbed = widen(absorbed)
        new_lat = widen(latents)
        new_rot = widen(ropes)
        cache_scores = (jnp.einsum('sqhc,stc->sqht', absorbed, slot_lat, precision=high) + jnp.einsum('sqhr,srt->sqht', query_rot, slot_rot, precision=high)) * scale
        valid = jnp.arange(CACHE, dtype=jnp.int32)[None, :] < slot_len[:, None]
        cache_scores = jnp.where(valid[:, None, None, :], cache_scores, -jnp.inf)
        new_scores = (jnp.einsum('sqhc,skc->sqhk', absorbed, new_lat, precision=high) + jnp.einsum('sqhr,skr->sqhk', query_rot, new_rot, precision=high)) * scale
        causal = jnp.arange(NEWTOK)[:, None] >= jnp.arange(NEWTOK)[None, :]
        new_scores = jnp.where(causal[None, :, None, :], new_scores, -jnp.inf)
        scores = jnp.concatenate([cache_scores, new_scores], axis=-1)
        largest = lax.optimization_barrier(jnp.max(scores, axis=-1, keepdims=True))
        expo = jnp.exp(scores - largest)
        weights = widen((expo / lax.optimization_barrier(jnp.sum(expo, axis=-1, keepdims=True))).astype(jnp.bfloat16))
        latent_out = jnp.einsum('sqht,stc->sqhc', weights[..., :CACHE], slot_lat, precision=high) + jnp.einsum('sqhk,skc->sqhc', weights[..., CACHE:], new_lat, precision=high)
        latent_out = widen(latent_out.astype(jnp.bfloat16))
        head_out = jnp.einsum('sqhc,chv->sqhv', latent_out, value_up, precision=high).astype(jnp.bfloat16)
        result = jnp.dot(head_out.reshape(SEQ_REP * NEWTOK, HEADS * VDIM), out_proj, preferred_element_type=jnp.float32)
        return result.astype(jnp.bfloat16).reshape(SEQ_REP, NEWTOK, D)
    outputs = lax.map(replica, (q_latent.reshape(REPLICAS, SEQ_REP, NEWTOK, QRANK), new_latent.reshape(REPLICAS, SEQ_REP, NEWTOK, KVRANK), new_rope.reshape(REPLICAS, SEQ_REP, NEWTOK, ROPE), cache_latent.reshape(REPLICAS, SEQ_REP, CACHE, KVRANK), cache_rope.reshape(REPLICAS, SEQ_REP, ROPE, CACHE), lengths.reshape(REPLICAS, SEQ_REP), assignment))
    return (outputs.reshape(SEQS, NEWTOK, D), weight_norm)
```

```python
import jax
import jax.numpy as jnp
from jax import lax
from jax.sharding import PartitionSpec as P

D = 7168
QRANK = 1536
KVRANK = 512
NOPE = 128
ROPE = 64
VDIM = 128
HEADS = 64
NEWTOK = 4
CACHE = 256


def widen(values):
    return lax.optimization_barrier(values).astype(jnp.float32)


def rotate_half(values, positions):
    half_width = values.shape[-1] // 2
    frequency = 10000.0 ** (-jnp.arange(half_width, dtype=jnp.float32) / half_width)
    angles = positions.astype(jnp.float32)[:, :, None, None] * frequency
    cosine = jnp.cos(angles)
    sine_part = jnp.sin(angles)
    lower_half = values[..., :half_width]
    upper_half = values[..., half_width:]
    return jnp.concatenate(
        [
            lower_half * cosine - upper_half * sine_part,
            upper_half * cosine + lower_half * sine_part,
        ],
        axis=-1,
    )


def shards(
    q_latent,
    new_latent,
    new_rope,
    cache_latent,
    cache_rope,
    lengths,
    assignment,
    w_uq,
    w_uk,
    w_uv,
    w_o,
):
    local_squares = (
        jnp.sum(w_uq * w_uq) + jnp.sum(w_uk * w_uk) + jnp.sum(w_uv * w_uv) + jnp.sum(w_o * w_o)
    )
    squares_total = lax.psum(local_squares, ("dp", "tp"))
    weight_norm = jnp.sqrt(squares_total / (HEADS * (NOPE + ROPE) + 2 * HEADS * NOPE + D)).reshape(
        1
    )
    query_cast = w_uq.astype(jnp.bfloat16)
    key_cast = w_uk.astype(jnp.bfloat16)
    value_cast = w_uv.astype(jnp.bfloat16)
    def regroup(block):
        mixed = lax.all_to_all(block, "tp", split_axis=1, concat_axis=0, tiled=True)
        return lax.all_gather(mixed, "dp", axis=0, tiled=True)

    query_up = regroup(query_cast)
    key_up = regroup(key_cast)
    value_up = regroup(value_cast)
    out_cast = w_o.astype(jnp.bfloat16)
    seq_count = q_latent.shape[0]
    heads_here = key_up.shape[1] // NOPE
    selector = (assignment[0][:, None] == jnp.arange(seq_count, dtype=jnp.int32)[None, :]).astype(
        jnp.bfloat16
    )

    def to_slots(array):
        moved = jnp.dot(
            selector.T, array.reshape(seq_count, -1), preferred_element_type=jnp.float32
        )
        return moved.astype(jnp.bfloat16).reshape(array.shape)

    query_slots = to_slots(q_latent)
    latent_slots = to_slots(new_latent)
    rope_slots = to_slots(new_rope)
    projected = jnp.dot(
        query_slots.reshape(seq_count * NEWTOK, QRANK), query_up, preferred_element_type=jnp.float32
    )
    projected = projected.astype(jnp.bfloat16).reshape(seq_count, NEWTOK, heads_here, NOPE + ROPE)
    query_nope = projected[..., :NOPE]
    positions = lengths[:, None] + jnp.arange(NEWTOK, dtype=jnp.int32)[None, :]
    query_rot = rotate_half(widen(projected[..., NOPE:]), positions).astype(jnp.bfloat16)
    absorbed = jnp.einsum(
        "sqhn,chn->sqhc",
        query_nope,
        key_up.reshape(KVRANK, heads_here, NOPE),
        preferred_element_type=jnp.float32,
    ).astype(jnp.bfloat16)
    scale = (NOPE + ROPE) ** (-0.5)
    cache_scores = jnp.einsum(
        "sqhc,stc->sqht", absorbed, cache_latent, preferred_element_type=jnp.float32
    )
    cache_scores = (
        cache_scores
        + jnp.einsum("sqhr,srt->sqht", query_rot, cache_rope, preferred_element_type=jnp.float32)
    ) * scale
    valid = jnp.arange(CACHE, dtype=jnp.int32)[None, :] < lengths[:, None]
    cache_scores = jnp.where(valid[:, None, None, :], cache_scores, -jnp.inf)
    new_scores = jnp.einsum(
        "sqhc,skc->sqhk", absorbed, latent_slots, preferred_element_type=jnp.float32
    )
    new_scores = (
        new_scores
        + jnp.einsum("sqhr,skr->sqhk", query_rot, rope_slots, preferred_element_type=jnp.float32)
    ) * scale
    causal = jnp.arange(NEWTOK)[:, None] >= jnp.arange(NEWTOK)[None, :]
    new_scores = jnp.where(causal[None, :, None, :], new_scores, -jnp.inf)
    scores = jnp.concatenate([cache_scores, new_scores], axis=-1)
    largest = jnp.max(scores, axis=-1, keepdims=True)
    expo = jnp.exp(scores - largest)
    weights = (expo / jnp.sum(expo, axis=-1, keepdims=True)).astype(jnp.bfloat16)
    latent_out = jnp.einsum(
        "sqht,stc->sqhc", weights[..., :CACHE], cache_latent, preferred_element_type=jnp.float32
    )
    latent_out = (
        latent_out
        + jnp.einsum(
            "sqhk,skc->sqhc", weights[..., CACHE:], latent_slots, preferred_element_type=jnp.float32
        )
    ).astype(jnp.bfloat16)
    head_out = jnp.einsum(
        "sqhc,chv->sqhv",
        latent_out,
        value_up.reshape(KVRANK, heads_here, VDIM),
        preferred_element_type=jnp.float32,
    ).astype(jnp.bfloat16)
    request_out = jnp.dot(
        selector, head_out.reshape(seq_count, -1), preferred_element_type=jnp.float32
    )
    request_out = request_out.astype(jnp.bfloat16).reshape(seq_count * NEWTOK, heads_here * VDIM)
    tp = lax.axis_size("tp")
    dp = lax.axis_size("dp")
    near = dp // tp
    out_rows = lax.all_to_all(out_cast, "tp", split_axis=0, concat_axis=1, tiled=True)
    near_groups = [[i * near + j for j in range(near)] for i in range(tp)]
    far_groups = [[i * near + j for i in range(tp)] for j in range(near)]
    out_block = lax.all_gather(
        out_rows, "dp", axis=1, tiled=True, axis_index_groups=near_groups
    )
    all_heads = lax.all_gather(
        request_out, "dp", axis=0, tiled=True, axis_index_groups=far_groups
    )
    partial_out = jnp.dot(all_heads, out_block, preferred_element_type=jnp.float32)
    reduced = lax.psum_scatter(
        partial_out.astype(jnp.bfloat16), "tp", scatter_dimension=0, tiled=True
    )
    pairs = []
    for i in range(tp):
        for j in range(near):
            for t in range(tp):
                pairs.append(((i * near + j) * tp + t, (t * near + j) * tp + i))
    moved = lax.ppermute(reduced, ("dp", "tp"), pairs)
    attention_out = moved.reshape(seq_count, NEWTOK, -1)
    return (attention_out, weight_norm)


def solution(mesh):
    in_specs = (
        P("dp", None, None),
        P("dp", None, None),
        P("dp", None, None),
        P("dp", None, None),
        P("dp", None, None),
        P("dp"),
        P("dp", None),
        P(("dp", "tp"), None),
        P(("dp", "tp"), None),
        P(("dp", "tp"), None),
        P(None, ("dp", "tp")),
    )
    out_specs = (P("dp", None, "tp"), P())
    return jax.shard_map(shards, mesh=mesh, in_specs=in_specs, out_specs=out_specs, check_vma=False)
```

```python
import functools

import jax
import jax.numpy as jnp
from jax import lax
from jax.experimental import pallas as pl
from jax.experimental.pallas import tpu as pltpu
from jax.sharding import PartitionSpec as P

D = 7168
QRANK = 1536
KVRANK = 512
NOPE = 128
ROPE = 64
VDIM = 128
HEADS = 64
NEWTOK = 4
CACHE = 256
CHUNKS = 2
GROUP = 4


def widen(values):
    return lax.optimization_barrier(values).astype(jnp.float32)


def rotate_half(values, positions):
    half_width = values.shape[-1] // 2
    frequency = 10000.0 ** (-jnp.arange(half_width, dtype=jnp.float32) / half_width)
    angles = positions.astype(jnp.float32)[:, :, None, None] * frequency
    cosine = jnp.cos(angles)
    sine_part = jnp.sin(angles)
    lower_half = values[..., :half_width]
    upper_half = values[..., half_width:]
    return jnp.concatenate(
        [
            lower_half * cosine - upper_half * sine_part,
            upper_half * cosine + lower_half * sine_part,
        ],
        axis=-1,
    )


def attention_kernel(
    heads, per_step, base, len_ref, query_ref, rot_ref, cache_ref, rope_ref, new_ref, new_rope_ref, out_ref
):
    scale = (NOPE + ROPE) ** (-0.5)
    rows = query_ref.shape[1]
    step = pl.program_id(0)
    slot = lax.broadcasted_iota(jnp.int32, (rows, CACHE), 1)
    token = lax.broadcasted_iota(jnp.int32, (rows, NEWTOK), 0) // heads
    other = lax.broadcasted_iota(jnp.int32, (rows, NEWTOK), 1)
    across = (((1,), (1,)), ((), ()))
    for group in range(0, per_step, GROUP):
        members = range(group, group + GROUP)
        raw = []
        for i in members:
            old_scores = lax.dot_general(
                query_ref[i], cache_ref[i], across, preferred_element_type=jnp.float32
            )
            old_scores += jnp.dot(rot_ref[i], rope_ref[i], preferred_element_type=jnp.float32)
            new_scores = lax.dot_general(
                query_ref[i], new_ref[i], across, preferred_element_type=jnp.float32
            )
            new_scores += lax.dot_general(
                rot_ref[i], new_rope_ref[i], across, preferred_element_type=jnp.float32
            )
            raw.append((old_scores, new_scores))
        weights = []
        for i, (old_scores, new_scores) in zip(members, raw):
            length = len_ref[base + step * per_step + i]
            old_scores = jnp.where(slot < length, old_scores * scale, -jnp.inf)
            new_scores = jnp.where(token >= other, new_scores * scale, -jnp.inf)
            largest = jnp.maximum(
                jnp.max(old_scores, axis=-1, keepdims=True),
                jnp.max(new_scores, axis=-1, keepdims=True),
            )
            old = jnp.exp(old_scores - largest)
            fresh = jnp.exp(new_scores - largest)
            total = jnp.sum(old, axis=-1, keepdims=True) + jnp.sum(fresh, axis=-1, keepdims=True)
            weights.append(
                ((old / total).astype(jnp.bfloat16), (fresh / total).astype(jnp.bfloat16))
            )
        mixed = []
        for i, (old, fresh) in zip(members, weights):
            result = jnp.dot(old, cache_ref[i], preferred_element_type=jnp.float32)
            result += jnp.dot(fresh, new_ref[i], preferred_element_type=jnp.float32)
            mixed.append(result.astype(jnp.bfloat16))
        for i, result in zip(members, mixed):
            out_ref[i] = result


def attend(heads, chunk, count, lengths, *arrays):
    per_step = 8
    first = chunk * count // per_step

    def spec(array):
        begin = 0 if array.shape[0] == count else first
        return pl.BlockSpec((per_step,) + array.shape[1:], lambda i: (begin + i, 0, 0))

    rows = arrays[0].shape[1]
    return pl.pallas_call(
        functools.partial(attention_kernel, heads, per_step, chunk * count),
        grid=(count // per_step,),
        out_shape=jax.ShapeDtypeStruct((count, rows, KVRANK), jnp.bfloat16),
        in_specs=[pl.BlockSpec(memory_space=pltpu.SMEM)] + [spec(array) for array in arrays],
        out_specs=pl.BlockSpec((per_step, rows, KVRANK), lambda i: (i, 0, 0)),
        compiler_params=pltpu.CompilerParams(vmem_limit_bytes=32 * 1024 * 1024),
        cost_estimate=pl.CostEstimate(
            flops=4 * count * rows * CACHE * KVRANK * 4,
            bytes_accessed=count * CACHE * KVRANK * 4,
            transcendentals=count * rows * CACHE,
        ),
        name="attend",
    )(lengths, *arrays)


def shards(
    q_latent,
    new_latent,
    new_rope,
    cache_latent,
    cache_rope,
    lengths,
    assignment,
    w_uq,
    w_uk,
    w_uv,
    w_o,
):
    local_squares = (
        jnp.sum(w_uq * w_uq) + jnp.sum(w_uk * w_uk) + jnp.sum(w_uv * w_uv) + jnp.sum(w_o * w_o)
    )
    squares_total = lax.psum(local_squares, ("dp", "tp"))
    tp = lax.axis_size("tp")
    dp = lax.axis_size("dp")
    near = dp // tp

    def swap(block):
        return lax.all_to_all(block, "tp", split_axis=1, concat_axis=0, tiled=True)

    def gather(block):
        return lax.all_gather(block, "dp", axis=0, tiled=True)

    query_mixed = swap(w_uq.astype(jnp.bfloat16))
    query_mixed, key_cast = lax.optimization_barrier((query_mixed, w_uk.astype(jnp.bfloat16)))
    key_mixed = swap(key_cast)
    key_mixed, value_cast, out_cast = lax.optimization_barrier(
        (key_mixed, w_uv.astype(jnp.bfloat16), w_o.astype(jnp.bfloat16))
    )
    value_mixed = swap(value_cast)
    query_up = gather(query_mixed)
    key_mixed, squares_total = lax.optimization_barrier((key_mixed, squares_total))
    query_up, key_mixed = lax.optimization_barrier((query_up, key_mixed))
    key_up = gather(key_mixed)
    out_rows = lax.all_to_all(out_cast, "tp", split_axis=0, concat_axis=1, tiled=True)
    key_up, value_mixed, out_rows = lax.optimization_barrier((key_up, value_mixed, out_rows))
    value_up = gather(value_mixed)
    width = out_rows.shape[1]
    place = lax.rem(lax.axis_index("dp"), near)
    out_block = lax.dynamic_update_slice(
        jnp.zeros((out_rows.shape[0], near * width), jnp.bfloat16), out_rows, (0, place * width)
    )
    for shift in range(1, near):
        pairs = [(d, d // near * near + (d + shift) % near) for d in range(dp)]
        arrived = lax.ppermute(out_rows, "dp", pairs)
        source = lax.rem(place + near - shift, near)
        out_block = lax.dynamic_update_slice(out_block, arrived, (0, source * width))
    seq_count = q_latent.shape[0]
    heads_here = key_up.shape[1] // NOPE
    selector = (assignment[0][:, None] == jnp.arange(seq_count, dtype=jnp.int32)[None, :]).astype(
        jnp.bfloat16
    )

    def to_slots(array):
        moved = jnp.dot(
            selector.T, array.reshape(seq_count, -1), preferred_element_type=jnp.float32
        )
        return moved.astype(jnp.bfloat16).reshape(array.shape)

    query_slots = to_slots(q_latent)
    latent_slots = to_slots(new_latent)
    rope_slots = to_slots(new_rope)
    weight_norm = jnp.sqrt(squares_total / (HEADS * (NOPE + ROPE) + 2 * HEADS * NOPE + D)).reshape(
        1
    )
    projected = jnp.dot(
        query_slots.reshape(seq_count * NEWTOK, QRANK), query_up, preferred_element_type=jnp.float32
    )
    projected = projected.astype(jnp.bfloat16).reshape(seq_count, NEWTOK, heads_here, NOPE + ROPE)
    query_nope = projected[..., :NOPE]
    positions = lengths[:, None] + jnp.arange(NEWTOK, dtype=jnp.int32)[None, :]
    query_rot = rotate_half(widen(projected[..., NOPE:]), positions).astype(jnp.bfloat16)
    ring = [(d, (d + near) % dp) for d in range(dp)]
    crossing = []
    for i in range(tp):
        for j in range(near):
            for t in range(tp):
                crossing.append(((i * near + j) * tp + t, (t * near + j) * tp + i))
    far = lax.axis_index("dp") // near
    value_heads = value_up.reshape(KVRANK, heads_here, VDIM)
    per_chunk = seq_count // CHUNKS
    key_heads = key_up.reshape(KVRANK, heads_here, NOPE)
    blocks = []
    for chunk in range(CHUNKS):
        rows = slice(chunk * per_chunk, (chunk + 1) * per_chunk)
        absorbed = jnp.einsum(
            "sqhn,chn->sqhc", query_nope[rows], key_heads, preferred_element_type=jnp.float32
        ).astype(jnp.bfloat16)
        latent_out = attend(
            heads_here,
            chunk,
            per_chunk,
            lengths,
            absorbed.reshape(per_chunk, NEWTOK * heads_here, KVRANK),
            query_rot[rows].reshape(per_chunk, NEWTOK * heads_here, ROPE),
            cache_latent,
            cache_rope,
            latent_slots,
            rope_slots,
        )
        head_out = jnp.einsum(
            "sqhc,chv->sqhv",
            latent_out.reshape(per_chunk, NEWTOK, heads_here, KVRANK),
            value_heads,
            preferred_element_type=jnp.float32,
        ).astype(jnp.bfloat16)
        blocks.append(head_out.reshape(per_chunk * NEWTOK, heads_here * VDIM))
    rows = per_chunk * NEWTOK
    partials = [jnp.zeros((tp * rows, near * width), jnp.bfloat16) for _ in blocks]
    arrived = [lax.ppermute(block, "dp", ring) for block in blocks]
    if CHUNKS > 1:
        arrived[0], blocks[-1] = lax.optimization_barrier((arrived[0], blocks[-1]))
    for step in range(tp):
        for chunk in range(CHUNKS):
            product = jnp.dot(blocks[chunk], out_block, preferred_element_type=jnp.float32)
            owner = lax.rem(far + tp - step, tp)
            partials[chunk] = lax.dynamic_update_slice(
                partials[chunk], product.astype(jnp.bfloat16), (owner * rows, 0)
            )
            if step < tp - 1:
                blocks[chunk] = arrived[chunk]
                if step < tp - 2:
                    arrived[chunk] = lax.ppermute(arrived[chunk], "dp", ring)
    pieces = []
    for partial_out in partials:
        reduced = lax.psum_scatter(partial_out, "tp", scatter_dimension=0, tiled=True)
        pieces.append(lax.ppermute(reduced, ("dp", "tp"), crossing))
    slot_out = jnp.concatenate(pieces, axis=0).reshape(seq_count, -1)
    attention_out = jnp.dot(selector, slot_out, preferred_element_type=jnp.float32)
    attention_out = attention_out.astype(jnp.bfloat16).reshape(seq_count, NEWTOK, -1)
    return (attention_out, weight_norm)


def solution(mesh):
    in_specs = (
        P("dp", None, None),
        P("dp", None, None),
        P("dp", None, None),
        P("dp", None, None),
        P("dp", None, None),
        P("dp"),
        P("dp", None),
        P(("dp", "tp"), None),
        P(("dp", "tp"), None),
        P(("dp", "tp"), None),
        P(None, ("dp", "tp")),
    )
    out_specs = (P("dp", None, "tp"), P())
    return jax.shard_map(shards, mesh=mesh, in_specs=in_specs, out_specs=out_specs, check_vma=False)
```
